512 devices in a mesh: sp: 64 (over z, y_hi, x), tp: 8 (over y_lo, core).
Axes of the slice: x: 4, y: 8 (y_hi: 2, y_lo: 4; y = y_hi * 4 + y_lo), z: 8, core: 2. Of those that a mesh axis runs over, the one named last changes fastest.
Arguments:
- fade_rate: float32 [1, 65536, 4096], P(None, 'sp', 'tp'), may hold values from 0.2 to 2
- update_in: bfloat16 [1, 65536, 4096], P(None, 'sp', 'tp'), may hold values from -6 to 6
- norm_gain: float32 [4096], P('tp'), may hold values from 0.25 to 1.75
Outputs:
- mixed_out: bfloat16 [1, 65536, 4096], P(None, 'sp', 'tp')
The draws below stay inside these ranges and needn't reach their ends.
All inputs are finite; a program needn't handle non-finite values.
Results may differ from the reference program's by a relative error of at most 0.0011.
Values sent between devices are 32-bit elements; how exact they have to be, the bound alone decides.
No kernel may reach another device: no remote copies, remote signals or barrier semaphores. Data moves between devices by JAX's collectives and lax.ppermute only.
A program may use at most 64 MiB of HBM per device.

```python
import jax
import jax.numpy as jnp
from jax import lax

BATCH = 1
CHANNELS = 4096
LENGTH = 65536


def steps_of(own_key, dims, split, smallest, top_value):
    def one(dim, parts):
        steps = jax.random.uniform(jax.random.fold_in(jax.random.fold_in(own_key, 6), dim), (parts,), jnp.float32, smallest / len(split), top_value / len(split))
        return jnp.repeat(jnp.exp(steps), dims[dim] // parts).reshape((-1,) + (1,) * (len(dims) - dim - 1))

    gain = one(*split[0])
    for cut in split[1:]:
        gain = gain * one(*cut)
    return gain


def normal_values(stream_key, shape, deviation, limit, pieces=(), kind=jnp.bfloat16):
    array = deviation * jax.random.normal(stream_key, shape, jnp.float32)
    if pieces:
        array = array * steps_of(stream_key, shape, pieces, -0.22, 0.18)
    return jnp.clip(array, -limit, limit).astype(kind)


def setup_inputs(seed: int = 0) -> dict:
    seeds = jax.random.split(jax.random.key(seed), 4)
    return {
        "fade_rate": jnp.clip(0.2 + 1.8 * jax.random.uniform(seeds[0], (BATCH, LENGTH, CHANNELS), jnp.float32) ** steps_of(seeds[0], (BATCH, LENGTH, CHANNELS), ((1, 64), (2, 8)), -0.2, 0.2), 0.2, 2.0),
        "update_in": normal_values(seeds[1], (BATCH, LENGTH, CHANNELS), 1.0, 6.0, ((1, 64), (2, 8))),
        "norm_gain": jnp.clip(1.0 + 0.15 * jax.random.normal(seeds[2], (CHANNELS,), jnp.float32), 0.25, 1.75),
    }


def join_pair(earlier, later):
    return (earlier[0] * later[0], later[0] * earlier[1] + later[1])

def reference(fade_rate, update_in, norm_gain):
    keep = jnp.exp(-fade_rate / LENGTH)
    push = update_in.astype(jnp.float32) * LENGTH ** (-0.5)
    forward = lax.associative_scan(join_pair, (keep, push), axis=1)[1]
    power = lax.optimization_barrier(jnp.mean(forward * forward, axis=-1, keepdims=True))
    mixed_out = (forward * lax.rsqrt(power + 1e-06) * norm_gain).astype(jnp.bfloat16)
    return mixed_out
```

```python
import functools
import math

import jax
import jax.numpy as jnp
from jax import lax
from jax.experimental import pallas as pl
from jax.experimental.pallas import tpu as pltpu
from jax.sharding import PartitionSpec as P

LANES = 128
F32, BF16 = jnp.float32, jnp.bfloat16
VMEM = pl.BlockSpec(memory_space=pltpu.VMEM)
HBM = pl.BlockSpec(memory_space=pltpu.HBM)
LOG2E = math.log2(math.e)


def pieces(x):
    high = x.astype(BF16)
    return high, (x - high.astype(F32)).astype(BF16)


def local_kernel(block, peers, rate, fade, update, decay, inner, message, fades, updates, sems):
    length, width = fade.shape
    blocks = length // block
    copies = []
    for b in range(blocks):
        rows = pl.ds(b * block, block)
        pair = (
            pltpu.make_async_copy(fade.at[rows], fades.at[rows], sems.at[0, b]),
            pltpu.make_async_copy(update.at[rows], updates.at[rows], sems.at[1, b]),
        )
        for copy in pair:
            copy.start()
        copies.append(pair)
    row = lax.broadcasted_iota(jnp.int32, (block, block), 0)
    column = lax.broadcasted_iota(jnp.int32, (block, block), 1)
    upto = jnp.where(column <= row, 1.0, 0.0).astype(BF16)

    def running(*terms):
        return sum(jnp.dot(upto, t, preferred_element_type=F32) for t in terms)

    faded = jnp.zeros((1, width), F32)
    pushed = jnp.zeros((1, width), F32)
    for b in range(blocks):
        rows = pl.ds(b * block, block)
        copies[b][0].wait()
        f = fades[rows, :]
        total = (running(*pieces(f)) + faded) * rate
        faded = faded + jnp.sum(f, axis=0, keepdims=True)
        decay[rows, :] = jnp.exp2(-total)
        growth = jnp.exp2(total) - 1.0
        copies[b][1].wait()
        u = updates[rows, :]
        so_far = running(u, *pieces(u.astype(F32) * growth)) + pushed
        inner[rows, :] = so_far
        pushed = so_far[block - 1 : block, :]
    cut = [slice(g * LANES, (g + 1) * LANES) for g in range(width // LANES)]
    tile = jnp.concatenate([faded[:, c] for c in cut] + [pushed[:, c] for c in cut], axis=0)
    for p in range(peers):
        message[p] = tile


def carry_kernel(rate, copies, tile, decay, inner, gathered, forward, message):
    length, width = decay.shape
    peers, high, lanes = gathered.shape
    groups = width // lanes
    me = lax.axis_index("sp")
    states, keeps = [], []
    for first in range(0, peers, 8):
        state = keep = None
        for p in range(first, first + 8):
            t = gathered[p]
            k = pltpu.roll(jnp.exp2(t * -rate), groups, 0)
            k = jnp.where(p < me, k, 1.0)
            t = jnp.where(p < me, t, 0.0)
            state = t * k if state is None else (state + t) * k
            keep = k if keep is None else keep * k
        states.append(state)
        keeps.append(keep)
    state = states[0]
    for s, k in zip(states[1:], keeps[1:]):
        state = state * k + s
    entering = [state[groups + g : groups + g + 1, :] for g in range(groups)]
    ones = jnp.ones((8, lanes), BF16)
    row = lax.broadcasted_iota(jnp.int32, (8, lanes), 0)
    out = jnp.zeros((8, lanes), F32)
    for s in range(length // lanes):
        rows = pl.ds(s * lanes, lanes)
        power = None
        for g in range(groups):
            at = pl.ds(g * lanes, lanes)
            f = decay[rows, at] * (inner[rows, at] + entering[g])
            forward[rows, at] = f
            power = f * f if power is None else power + f * f
        sums = sum(
            lax.dot_general(ones, t, (((1,), (1,)), ((), ())), preferred_element_type=F32)
            for t in pieces(power)
        )
        out = jnp.where(row == s, sums, out)
    for p in range(copies):
        message[p] = out


def norm_kernel(channels, total_length, forward, powers, gain, out, staged, sems):
    length, width = forward.shape
    lanes = powers.shape[-1]
    power = powers[0]
    for p in range(1, powers.shape[0]):
        power = power + powers[p]
    scale = lax.rsqrt(power * (1.0 / (channels * total_length)) + 1e-06) * total_length ** (-0.5)
    scale = scale.T
    copies = []
    for s in range(length // lanes):
        rows = pl.ds(s * lanes, lanes)
        staged[rows, :] = (forward[rows, :] * scale[:, s : s + 1] * gain[...]).astype(BF16)
        copies.append(pltpu.make_async_copy(staged.at[rows], out.at[rows], sems.at[s]))
        copies[-1].start()
    for copy in copies:
        copy.wait()


def per_device(fade_rate, update_in, norm_gain):
    _, length, width = fade_rate.shape
    stretches, parts = lax.axis_size("sp"), lax.axis_size("tp")
    total_length = length * stretches
    rate = LOG2E / total_length
    block = 256
    blocks = length // block
    limit = pltpu.CompilerParams(vmem_limit_bytes=24 * 1024 * 1024)
    wide = jax.ShapeDtypeStruct((length, width), F32)
    decay, inner, summary = pl.pallas_call(
        functools.partial(local_kernel, block, stretches, rate),
        out_shape=(wide, wide, jax.ShapeDtypeStruct((stretches, 8, LANES), F32)),
        in_specs=[HBM, HBM],
        out_specs=(VMEM, VMEM, VMEM),
        scratch_shapes=[
            pltpu.VMEM((length, width), F32),
            pltpu.VMEM((length, width), BF16),
            pltpu.SemaphoreType.DMA((2, blocks)),
        ],
        compiler_params=limit,
        name="local",
    )(*(pltpu.with_memory_space_constraint(a[0], pltpu.HBM) for a in (fade_rate, update_in)))
    gathered = lax.all_to_all(summary, "sp", 0, 0, tiled=True)
    forward, power = pl.pallas_call(
        functools.partial(carry_kernel, rate, parts, 8),
        out_shape=(wide, jax.ShapeDtypeStruct((parts, 8, LANES), F32)),
        in_specs=[VMEM, VMEM, VMEM],
        out_specs=(VMEM, VMEM),
        compiler_params=limit,
        name="carry",
    )(decay, inner, gathered)
    powers = lax.all_to_all(power, "tp", 0, 0, tiled=True)
    out = pl.pallas_call(
        functools.partial(norm_kernel, width * parts, total_length),
        out_shape=jax.ShapeDtypeStruct((length, width), BF16),
        in_specs=[VMEM, VMEM, VMEM],
        out_specs=HBM,
        scratch_shapes=[
            pltpu.VMEM((length, width), BF16),
            pltpu.SemaphoreType.DMA((length // LANES,)),
        ],
        compiler_params=limit,
        name="norm",
    )(forward, powers, norm_gain[None])
    return out[None]


def solution(mesh):
    placed = (P(None, "sp", "tp"), P(None, "sp", "tp"), P("tp"))
    return jax.shard_map(
        per_device, mesh=mesh, in_specs=placed, out_specs=P(None, "sp", "tp"), check_vma=False
    )
```

```python
import functools
import math

import jax
import jax.numpy as jnp
from jax import lax
from jax.experimental import pallas as pl
from jax.experimental.pallas import tpu as pltpu
from jax.sharding import PartitionSpec as P

LANES = 128
F32, BF16 = jnp.float32, jnp.bfloat16
VMEM = pl.BlockSpec(memory_space=pltpu.VMEM)
HBM = pl.BlockSpec(memory_space=pltpu.HBM)
LOG2E = math.log2(math.e)


def pieces(x):
    high = x.astype(BF16)
    return high, (x - high.astype(F32)).astype(BF16)


def as_tile(*rows):
    lines = [r[:, at : at + LANES] for r in rows for at in range(0, r.shape[1], LANES)]
    return jnp.concatenate(lines, axis=0)


def local_kernel(block, stage, rate, fade, update, decay, inner, marks, message, fades, updates, sems):
    length, width = fade.shape
    half = 2 * LANES
    copies = []
    for b in range(length // stage):
        rows = pl.ds(b * stage, stage)
        pair = (
            pltpu.make_async_copy(fade.at[rows], fades.at[rows], sems.at[0, b]),
            pltpu.make_async_copy(update.at[rows], updates.at[rows], sems.at[1, b]),
        )
        for copy in pair:
            copy.start()
        copies.append(pair)
    row = lax.broadcasted_iota(jnp.int32, (block, block), 0)
    column = lax.broadcasted_iota(jnp.int32, (block, block), 1)
    upto = jnp.where(column <= row, 1.0, 0.0).astype(BF16)
    twice = jnp.concatenate([upto, upto], axis=1)

    kept, ended = None, None
    for b in range(length // block):
        rows = pl.ds(b * block, block)
        if b * block % stage == 0:
            for copy in copies[b * block // stage]:
                copy.wait()
        keeps, ends = [], []
        for h in range(width // half):
            at = pl.ds(h * half, half)
            f = fades[rows, at]
            total = jnp.dot(upto, f.astype(BF16), preferred_element_type=F32) * rate
            decay[rows, at] = jnp.exp2(-total)
            u = updates[rows, at]
            more = (u.astype(F32) * (jnp.exp2(total) - 1.0)).astype(BF16)
            so_far = jnp.dot(twice, jnp.concatenate([u, more], axis=0), preferred_element_type=F32)
            inner[rows, at] = so_far
            keep = jnp.exp2(jnp.sum(f, axis=0, keepdims=True) * -rate)
            keeps.append(keep)
            ends.append(so_far[block - 1 :, :] * keep)
        keep, end = (jnp.concatenate(r, axis=1) for r in (keeps, ends))
        marks[b] = as_tile(keep, end)
        kept, ended = (keep, end) if kept is None else (kept * keep, ended * keep + end)
    tile = as_tile(kept, ended)
    for p in range(message.shape[0]):
        message[p] = tile


def carry_kernel(decay, inner, marks, gathered, forward, message):
    length, width = decay.shape
    peers, high, lanes = gathered.shape
    groups = width // lanes
    blocks = marks.shape[0]
    block = length // blocks
    row = lax.broadcasted_iota(jnp.int32, (high, lanes), 0)
    earlier = jnp.where(row >= groups, lax.axis_index("sp"), 0)
    states, keeps = [], []
    for first in range(0, peers, 8):
        state = keep = None
        for p in range(first, first + 8):
            t = gathered[p]
            k = jnp.where(p < earlier, pltpu.roll(t, groups, 0), 1.0)
            t = jnp.where(p < earlier, t, 0.0)
            state = t if state is None else state * k + t
            keep = k if keep is None else keep * k
        states.append(state)
        keeps.append(keep)
    state = states[0]
    for s, k in zip(states[1:], keeps[1:]):
        state = state * k + s
    ones = jnp.ones((8, lanes), BF16)
    out = jnp.zeros((8, lanes), F32)
    for b in range(blocks):
        rows = pl.ds(b * block, block)
        power = None
        for g in range(groups):
            at = pl.ds(g * lanes, lanes)
            f = decay[rows, at] * (inner[rows, at] + state[groups + g : groups + g + 1, :])
            forward[rows, at] = f
            power = f * f if power is None else power + f * f
        sums = sum(
            lax.dot_general(ones, t, (((1,), (1,)), ((), ())), preferred_element_type=F32)
            for t in pieces(power)
        )
        out = jnp.where(row == b, sums, out)
        state = state * pltpu.roll(marks[b], groups, 0) + marks[b]
    for p in range(message.shape[0]):
        message[p] = out


def norm_kernel(channels, total_length, forward, powers, gain, out, staged, sems):
    length, width = forward.shape
    lanes = powers.shape[-1]
    power = powers[0]
    for p in range(1, powers.shape[0]):
        power = power + powers[p]
    scale = lax.rsqrt(power * (1.0 / (channels * total_length)) + 1e-06) * total_length ** (-0.5)
    scale = scale.T
    copies = []
    for s in range(length // lanes):
        rows = pl.ds(s * lanes, lanes)
        staged[rows, :] = (forward[rows, :] * scale[:, s : s + 1] * gain[...]).astype(BF16)
        copies.append(pltpu.make_async_copy(staged.at[rows], out.at[rows], sems.at[s]))
        copies[-1].start()
    for copy in copies:
        copy.wait()


def per_device(fade_rate, update_in, norm_gain):
    _, length, width = fade_rate.shape
    stretches, parts = lax.axis_size("sp"), lax.axis_size("tp")
    total_length = length * stretches
    rate = LOG2E / total_length
    block, stage = LANES, 512
    blocks = length // block
    limit = pltpu.CompilerParams(vmem_limit_bytes=24 * 1024 * 1024)
    wide = jax.ShapeDtypeStruct((length, width), F32)

    def tiles(count):
        return jax.ShapeDtypeStruct((count, 8, LANES), F32)

    decay, inner, marks, summary = pl.pallas_call(
        functools.partial(local_kernel, block, stage, rate),
        out_shape=(wide, wide, tiles(blocks), tiles(stretches)),
        in_specs=[HBM, HBM],
        out_specs=(VMEM, VMEM, VMEM, VMEM),
        scratch_shapes=[
            pltpu.VMEM((length, width), F32),
            pltpu.VMEM((length, width), BF16),
            pltpu.SemaphoreType.DMA((2, length // stage)),
        ],
        compiler_params=limit,
        name="local",
    )(*(pltpu.with_memory_space_constraint(a[0], pltpu.HBM) for a in (fade_rate, update_in)))
    gathered = lax.all_to_all(summary, "sp", 0, 0, tiled=True)
    forward, power = pl.pallas_call(
        carry_kernel,
        out_shape=(wide, tiles(parts)),
        in_specs=[VMEM, VMEM, VMEM, VMEM],
        out_specs=(VMEM, VMEM),
        compiler_params=limit,
        name="carry",
    )(decay, inner, marks, gathered)
    powers = lax.all_to_all(power, "tp", 0, 0, tiled=True)
    out = pl.pallas_call(
        functools.partial(norm_kernel, width * parts, total_length),
        out_shape=jax.ShapeDtypeStruct((length, width), BF16),
        in_specs=[VMEM, VMEM, VMEM],
        out_specs=HBM,
        scratch_shapes=[
            pltpu.VMEM((length, width), BF16),
            pltpu.SemaphoreType.DMA((length // LANES,)),
        ],
        compiler_params=limit,
        name="norm",
    )(forward, powers, norm_gain[None])
    return out[None]


def solution(mesh):
    placed = (P(None, "sp", "tp"), P(None, "sp", "tp"), P("tp"))
    return jax.shard_map(
        per_device, mesh=mesh, in_specs=placed, out_specs=P(None, "sp", "tp"), check_vma=False
    )
```

```python
import functools
import math

import jax
import jax.numpy as jnp
from jax import lax
from jax.experimental import pallas as pl
from jax.experimental.pallas import tpu as pltpu
from jax.sharding import PartitionSpec as P

LANES = 128
F32, BF16 = jnp.float32, jnp.bfloat16
VMEM = pl.BlockSpec(memory_space=pltpu.VMEM)
HBM = pl.BlockSpec(memory_space=pltpu.HBM)
LOG2E = math.log2(math.e)


def pieces(x):
    high = x.astype(BF16)
    return high, (x - high.astype(F32)).astype(BF16)


def as_tile(*rows):
    lines = [r[:, at : at + LANES] for r in rows for at in range(0, r.shape[1], LANES)]
    return jnp.concatenate(lines, axis=0)


def local_kernel(block, stage, rate, fade, update, drop, inner, marks, message, fades, updates, sems):
    length, width = fade.shape
    half = 2 * LANES
    copies = []
    for b in range(length // stage):
        rows = pl.ds(b * stage, stage)
        pair = (
            pltpu.make_async_copy(fade.at[rows], fades.at[rows], sems.at[0, b]),
            pltpu.make_async_copy(update.at[rows], updates.at[rows], sems.at[1, b]),
        )
        for copy in pair:
            copy.start()
        copies.append(pair)
    row = lax.broadcasted_iota(jnp.int32, (block, block), 0)
    column = lax.broadcasted_iota(jnp.int32, (block, block), 1)
    upto = jnp.where(column <= row, 1.0, 0.0).astype(BF16)
    twice = jnp.concatenate([upto, upto], axis=1)

    kept, ended = None, None
    for b in range(length // block):
        rows = pl.ds(b * block, block)
        if b * block % stage == 0:
            for copy in copies[b * block // stage]:
                copy.wait()
        keeps, ends = [], []
        for h in range(width // half):
            at = pl.ds(h * half, half)
            f = fades[rows, at]
            total = jnp.dot(upto, f.astype(BF16), preferred_element_type=F32) * rate
            drop[rows, at] = (jnp.exp2(-total) - 1.0).astype(BF16)
            u = updates[rows, at]
            more = (u.astype(F32) * (jnp.exp2(total) - 1.0)).astype(BF16)
            so_far = jnp.dot(twice, jnp.concatenate([u, more], axis=0), preferred_element_type=F32)
            inner[rows, at] = so_far
            keep = jnp.exp2(jnp.sum(f, axis=0, keepdims=True) * -rate)
            keeps.append(keep)
            ends.append(so_far[block - 1 :, :] * keep)
        keep, end = (jnp.concatenate(r, axis=1) for r in (keeps, ends))
        marks[b] = as_tile(keep, end)
        kept, ended = (keep, end) if kept is None else (kept * keep, ended * keep + end)
    message[...] = as_tile(kept, ended)


def prefix_kernel(axis, gathered, keep, end, total):
    peers, high, lanes = gathered.shape
    row = lax.broadcasted_iota(jnp.int32, (high, lanes), 0)
    before = jnp.where(row >= high // 2, lax.rem(lax.axis_index(axis), peers), 0)
    counted = jnp.where(row >= high // 2, peers, 0)
    own, whole = [], []
    for first in range(0, peers, 8):
        for count, links in ((before, own), (counted, whole)):
            kept = ended = None
            for p in range(first, min(first + 8, peers)):
                t = gathered[p]
                k = jnp.where(p < count, pltpu.roll(t, high // 2, 0), 1.0)
                t = jnp.where(p < count, t, 0.0)
                ended = t if ended is None else ended * k + t
                kept = k if kept is None else kept * k
            links.append((kept, ended))
    kept, ended = own[0]
    for k, e in own[1:]:
        kept, ended = kept * k, ended * k + e
    keep[...] = kept
    end[...] = ended
    ended = whole[0][1]
    for k, e in whole[1:]:
        ended = ended * k + e
    total[...] = ended


def carry_kernel(drop, inner, marks, keep, end, start, forward, message):
    length, width = drop.shape
    blocks, _, lanes = marks.shape
    groups = width // lanes
    block = length // blocks
    row = lax.broadcasted_iota(jnp.int32, (8, lanes), 0)
    state = start[...] * keep[...] + end[...]
    ones = jnp.ones((8, lanes), BF16)
    out = jnp.zeros((8, lanes), F32)
    for b in range(blocks):
        rows = pl.ds(b * block, block)
        power = None
        for g in range(groups):
            at = pl.ds(g * lanes, lanes)
            f = inner[rows, at] + state[groups + g : groups + g + 1, :]
            f = f + f * drop[rows, at].astype(F32)
            forward[rows, at] = f
            power = f * f if power is None else power + f * f
        sums = sum(
            lax.dot_general(ones, t, (((1,), (1,)), ((), ())), preferred_element_type=F32)
            for t in pieces(power)
        )
        out = jnp.where(row == b, sums, out)
        state = state * pltpu.roll(marks[b], groups, 0) + marks[b]
    for p in range(message.shape[0]):
        message[p] = out


def norm_kernel(channels, total_length, forward, powers, gain, out, staged, sems):
    length, width = forward.shape
    lanes = powers.shape[-1]
    power = powers[0]
    for p in range(1, powers.shape[0]):
        power = power + powers[p]
    scale = lax.rsqrt(power * (1.0 / (channels * total_length)) + 1e-06) * total_length ** (-0.5)
    scale = scale.T
    copies = []
    for s in range(length // lanes):
        rows = pl.ds(s * lanes, lanes)
        staged[rows, :] = (forward[rows, :] * scale[:, s : s + 1] * gain[...]).astype(BF16)
        copies.append(pltpu.make_async_copy(staged.at[rows], out.at[rows], sems.at[s]))
        copies[-1].start()
    for copy in copies:
        copy.wait()


def per_device(fade_rate, update_in, norm_gain):
    _, length, width = fade_rate.shape
    stretches, parts = lax.axis_size("sp"), lax.axis_size("tp")
    total_length = length * stretches
    rate = LOG2E / total_length
    block, stage = LANES, 512
    half = stretches // 2
    blocks = length // block
    limit = pltpu.CompilerParams(vmem_limit_bytes=24 * 1024 * 1024)
    wide = jax.ShapeDtypeStruct((length, width), F32)

    def tiles(count):
        return jax.ShapeDtypeStruct((count, 8, LANES), F32)

    tile = jax.ShapeDtypeStruct((8, LANES), F32)
    drop, inner, marks, summary = pl.pallas_call(
        functools.partial(local_kernel, block, stage, rate),
        out_shape=(jax.ShapeDtypeStruct((length, width), BF16), wide, tiles(blocks), tile),
        in_specs=[HBM, HBM],
        out_specs=(VMEM,) * 4,
        scratch_shapes=[
            pltpu.VMEM((length, width), F32),
            pltpu.VMEM((length, width), BF16),
            pltpu.SemaphoreType.DMA((2, length // stage)),
        ],
        compiler_params=limit,
        name="local",
    )(*(pltpu.with_memory_space_constraint(a[0], pltpu.HBM) for a in (fade_rate, update_in)))
    prefix = pl.pallas_call(
        functools.partial(prefix_kernel, "sp"),
        out_shape=(tile,) * 3,
        in_specs=[VMEM],
        out_specs=(VMEM,) * 3,
        compiler_params=limit,
        name="prefix",
    )
    early = lax.axis_index("sp") < half
    halves = [list(range(half)), list(range(half, stretches))]

    def within_half(summary):
        copies = jnp.broadcast_to(summary, (half, *summary.shape))
        gathered = lax.all_to_all(copies, "sp", 0, 0, axis_index_groups=halves, tiled=True)
        return prefix(gathered)

    keep, end, total = lax.cond(
        early, within_half, lambda s: (jnp.zeros_like(s),) * 3, summary
    )
    start = lax.ppermute(total, "sp", [(i, stretches - 1 - i) for i in range(half)])
    keep, end = lax.cond(
        early, lambda s, *found: found, lambda s, *_: within_half(s)[:2], summary, keep, end
    )
    forward, power = pl.pallas_call(
        carry_kernel,
        out_shape=(wide, tiles(parts)),
        in_specs=[VMEM] * 6,
        out_specs=(VMEM, VMEM),
        compiler_params=limit,
        name="carry",
    )(drop, inner, marks, keep, end, start)
    powers = lax.all_to_all(power, "tp", 0, 0, tiled=True)
    out = pl.pallas_call(
        functools.partial(norm_kernel, width * parts, total_length),
        out_shape=jax.ShapeDtypeStruct((length, width), BF16),
        in_specs=[VMEM, VMEM, VMEM],
        out_specs=HBM,
        scratch_shapes=[
            pltpu.VMEM((length, width), BF16),
            pltpu.SemaphoreType.DMA((length // LANES,)),
        ],
        compiler_params=limit,
        name="norm",
    )(forward, powers, norm_gain[None])
    return out[None]


def solution(mesh):
    placed = (P(None, "sp", "tp"), P(None, "sp", "tp"), P("tp"))
    return jax.shard_map(
        per_device, mesh=mesh, in_specs=placed, out_specs=P(None, "sp", "tp"), check_vma=False
    )
```

```python
import functools
import math

import jax
import jax.numpy as jnp
from jax import lax
from jax.experimental import pallas as pl
from jax.experimental.pallas import tpu as pltpu
from jax.sharding import PartitionSpec as P

LANES = 128
F32, BF16 = jnp.float32, jnp.bfloat16
VMEM = pl.BlockSpec(memory_space=pltpu.VMEM)
HBM = pl.BlockSpec(memory_space=pltpu.HBM)
LOG2E = math.log2(math.e)


def pieces(x):
    high = x.astype(BF16)
    return high, (x - high.astype(F32)).astype(BF16)


def as_tile(*rows):
    lines = [r[:, at : at + LANES] for r in rows for at in range(0, r.shape[1], LANES)]
    return jnp.concatenate(lines, axis=0)


def local_kernel(block, stage, rate, fade, update, drop, inner, marks, message, fades, updates, sems):
    length, width = fade.shape
    half = 2 * LANES
    copies = []
    for b in range(length // stage):
        rows = pl.ds(b * stage, stage)
        pair = (
            pltpu.make_async_copy(fade.at[rows], fades.at[rows], sems.at[0, b]),
            pltpu.make_async_copy(update.at[rows], updates.at[rows], sems.at[1, b]),
        )
        for copy in pair:
            copy.start()
        copies.append(pair)
    row = lax.broadcasted_iota(jnp.int32, (block, block), 0)
    column = lax.broadcasted_iota(jnp.int32, (block, block), 1)
    upto = jnp.where(column <= row, 1.0, 0.0).astype(BF16)
    twice = jnp.concatenate([upto, upto], axis=1)

    kept, ended = None, None
    for b in range(length // block):
        rows = pl.ds(b * block, block)
        if b * block % stage == 0:
            for copy in copies[b * block // stage]:
                copy.wait()
        keeps, ends = [], []
        for h in range(width // half):
            at = pl.ds(h * half, half)
            f = fades[rows, at]
            total = jnp.dot(upto, f.astype(BF16), preferred_element_type=F32) * rate
            drop[rows, at] = (jnp.exp2(-total) - 1.0).astype(BF16)
            u = updates[rows, at]
            more = (u.astype(F32) * (jnp.exp2(total) - 1.0)).astype(BF16)
            so_far = jnp.dot(twice, jnp.concatenate([u, more], axis=0), preferred_element_type=F32)
            inner[rows, at] = so_far
            keep = jnp.exp2(jnp.sum(f, axis=0, keepdims=True) * -rate)
            keeps.append(keep)
            ends.append(so_far[block - 1 :, :] * keep)
        keep, end = (jnp.concatenate(r, axis=1) for r in (keeps, ends))
        marks[b] = as_tile(keep, end)
        kept, ended = (keep, end) if kept is None else (kept * keep, ended * keep + end)
    message[...] = as_tile(kept, ended)


def prefix_kernel(axis, gathered, keep, end, *whole):
    peers, high, lanes = gathered.shape
    row = lax.broadcasted_iota(jnp.int32, (high, lanes), 0)
    before = jnp.where(row >= high // 2, lax.rem(lax.axis_index(axis), peers), 0)
    counts = [before] + [jnp.where(row >= high // 2, peers, 0)] * bool(whole)
    found = [[] for _ in counts]
    for first in range(0, peers, 8):
        for count, links in zip(counts, found):
            kept = ended = None
            for p in range(first, min(first + 8, peers)):
                t = gathered[p]
                k = jnp.where(p < count, pltpu.roll(t, high // 2, 0), 1.0)
                t = jnp.where(p < count, t, 0.0)
                ended = t if ended is None else ended * k + t
                kept = k if kept is None else kept * k
            links.append((kept, ended))
    for links, out in zip(found, ((keep, end), whole)):
        kept, ended = links[0]
        for k, e in links[1:]:
            kept, ended = kept * k, ended * k + e
        for ref, value in zip(out[::-1], (ended, kept)):
            ref[...] = value


def carry_kernel(drop, inner, marks, keep, end, *rest):
    *starts, forward, message = rest
    length, width = drop.shape
    blocks, _, lanes = marks.shape
    groups = width // lanes
    block = length // blocks
    row = lax.broadcasted_iota(jnp.int32, (8, lanes), 0)
    state = sum(start[...] for start in starts) * keep[...] + end[...]
    ones = jnp.ones((8, lanes), BF16)
    out = jnp.zeros((8, lanes), F32)
    for b in range(blocks):
        rows = pl.ds(b * block, block)
        power = None
        for g in range(groups):
            at = pl.ds(g * lanes, lanes)
            f = inner[rows, at] + state[groups + g : groups + g + 1, :]
            f = f + f * drop[rows, at].astype(F32)
            forward[rows, at] = f
            power = f * f if power is None else power + f * f
        sums = sum(
            lax.dot_general(ones, t, (((1,), (1,)), ((), ())), preferred_element_type=F32)
            for t in pieces(power)
        )
        out = jnp.where(row == b, sums, out)
        state = state * pltpu.roll(marks[b], groups, 0) + marks[b]
    for p in range(message.shape[0]):
        message[p] = out


def norm_kernel(channels, total_length, forward, powers, gain, out, staged, sems):
    length, width = forward.shape
    lanes = powers.shape[-1]
    power = powers[0]
    for p in range(1, powers.shape[0]):
        power = power + powers[p]
    scale = lax.rsqrt(power * (1.0 / (channels * total_length)) + 1e-06) * total_length ** (-0.5)
    scale = scale.T
    copies = []
    for s in range(length // lanes):
        rows = pl.ds(s * lanes, lanes)
        staged[rows, :] = (forward[rows, :] * scale[:, s : s + 1] * gain[...]).astype(BF16)
        copies.append(pltpu.make_async_copy(staged.at[rows], out.at[rows], sems.at[s]))
        copies[-1].start()
    for copy in copies:
        copy.wait()


def per_device(fade_rate, update_in, norm_gain):
    _, length, width = fade_rate.shape
    stretches, parts = lax.axis_size("sp"), lax.axis_size("tp")
    total_length = length * stretches
    rate = LOG2E / total_length
    block, stage = LANES, 512
    half, quarter = stretches // 2, stretches // 4
    blocks = length // block
    limit = pltpu.CompilerParams(vmem_limit_bytes=24 * 1024 * 1024)
    wide = jax.ShapeDtypeStruct((length, width), F32)

    def tiles(count):
        return jax.ShapeDtypeStruct((count, 8, LANES), F32)

    tile = jax.ShapeDtypeStruct((8, LANES), F32)
    drop, inner, marks, summary = pl.pallas_call(
        functools.partial(local_kernel, block, stage, rate),
        out_shape=(jax.ShapeDtypeStruct((length, width), BF16), wide, tiles(blocks), tile),
        in_specs=[HBM, HBM],
        out_specs=(VMEM,) * 4,
        scratch_shapes=[
            pltpu.VMEM((length, width), F32),
            pltpu.VMEM((length, width), BF16),
            pltpu.SemaphoreType.DMA((2, length // stage)),
        ],
        compiler_params=limit,
        name="local",
    )(*(pltpu.with_memory_space_constraint(a[0], pltpu.HBM) for a in (fade_rate, update_in)))
    me = lax.axis_index("sp")

    def within(size, whole):
        groups = [list(range(at, at + size)) for at in range(0, stretches, size)]
        prefix = pl.pallas_call(
            functools.partial(prefix_kernel, "sp"),
            out_shape=(tile,) * (2 + whole),
            in_specs=[VMEM],
            out_specs=(VMEM,) * (2 + whole),
            compiler_params=limit,
            name="prefix",
        )

        def found(summary, *_):
            copies = jnp.broadcast_to(summary, (size, *summary.shape))
            return prefix(
                lax.all_to_all(copies, "sp", 0, 0, axis_index_groups=groups, tiled=True)
            )

        return found

    none = jnp.zeros((8, LANES), F32)
    keep, end, first = lax.cond(
        me < quarter, within(quarter, 1), lambda *_: (none,) * 3, summary
    )
    handed = [lax.ppermute(first, "sp", [(i, i + quarter) for i in range(quarter)])]
    keep, end, kept, ended = lax.cond(
        me // quarter == 1,
        within(quarter, 2),
        lambda _, *found: (*found, none, none),
        summary,
        keep,
        end,
    )
    second = handed[0] * kept + ended
    for pairs in (
        [(quarter + i, 2 * quarter + i) for i in range(quarter)],
        [(quarter + i, 3 * quarter + (i + quarter // 2) % quarter) for i in range(quarter)],
    ):
        handed.append(lax.ppermute(second, "sp", pairs))
    keep, end = lax.cond(
        me >= half, within(half, 0), lambda _, *found: found, summary, keep, end
    )
    forward, power = pl.pallas_call(
        carry_kernel,
        out_shape=(wide, tiles(parts)),
        in_specs=[VMEM] * 8,
        out_specs=(VMEM, VMEM),
        compiler_params=limit,
        name="carry",
    )(drop, inner, marks, keep, end, *handed)
    powers = lax.all_to_all(power, "tp", 0, 0, tiled=True)
    out = pl.pallas_call(
        functools.partial(norm_kernel, width * parts, total_length),
        out_shape=jax.ShapeDtypeStruct((length, width), BF16),
        in_specs=[VMEM, VMEM, VMEM],
        out_specs=HBM,
        scratch_shapes=[
            pltpu.VMEM((length, width), BF16),
            pltpu.SemaphoreType.DMA((length // LANES,)),
        ],
        compiler_params=limit,
        name="norm",
    )(forward, powers, norm_gain[None])
    return out[None]


def solution(mesh):
    placed = (P(None, "sp", "tp"), P(None, "sp", "tp"), P("tp"))
    return jax.shard_map(
        per_device, mesh=mesh, in_specs=placed, out_specs=P(None, "sp", "tp"), check_vma=False
    )
```

```python
import functools
import math

import jax
import jax.numpy as jnp
from jax import lax
from jax.experimental import pallas as pl
from jax.experimental.pallas import tpu as pltpu
from jax.sharding import PartitionSpec as P

LANES = 128
F32, BF16 = jnp.float32, jnp.bfloat16
VMEM = pl.BlockSpec(memory_space=pltpu.VMEM)
HBM = pl.BlockSpec(memory_space=pltpu.HBM)
LOG2E = math.log2(math.e)


def pieces(x):
    high = x.astype(BF16)
    return high, (x - high.astype(F32)).astype(BF16)


def as_tile(*rows):
    lines = [r[:, at : at + LANES] for r in rows for at in range(0, r.shape[1], LANES)]
    return jnp.concatenate(lines, axis=0)


def local_kernel(block, stage, rate, fade, update, drop, inner, marks, message, fades, updates, sems):
    length, width = fade.shape
    half = 2 * LANES
    copies = []
    for b in range(length // stage):
        rows = pl.ds(b * stage, stage)
        pair = (
            pltpu.make_async_copy(fade.at[rows], fades.at[rows], sems.at[0, b]),
            pltpu.make_async_copy(update.at[rows], updates.at[rows], sems.at[1, b]),
        )
        for copy in pair:
            copy.start()
        copies.append(pair)
    row = lax.broadcasted_iota(jnp.int32, (block, block), 0)
    column = lax.broadcasted_iota(jnp.int32, (block, block), 1)
    upto = jnp.where(column <= row, 1.0, 0.0).astype(BF16)
    twice = jnp.concatenate([upto, upto], axis=1)

    kept, ended = None, None
    for b in range(length // block):
        rows = pl.ds(b * block, block)
        if b * block % stage == 0:
            for copy in copies[b * block // stage]:
                copy.wait()
        keeps, ends = [], []
        for h in range(width // half):
            at = pl.ds(h * half, half)
            f = fades[rows, at]
            total = jnp.dot(upto, f.astype(BF16), preferred_element_type=F32) * rate
            drop[rows, at] = (jnp.exp2(-total) - 1.0).astype(BF16)
            u = updates[rows, at]
            more = (u.astype(F32) * (jnp.exp2(total) - 1.0)).astype(BF16)
            so_far = jnp.dot(twice, jnp.concatenate([u, more], axis=0), preferred_element_type=F32)
            inner[rows, at] = so_far
            keep = jnp.exp2(jnp.sum(f, axis=0, keepdims=True) * -rate)
            keeps.append(keep)
            ends.append(so_far[block - 1 :, :] * keep)
        keep, end = (jnp.concatenate(r, axis=1) for r in (keeps, ends))
        marks[b] = as_tile(keep, end)
        kept, ended = (keep, end) if kept is None else (kept * keep, ended * keep + end)
    message[...] = as_tile(kept, ended)


def prefix_kernel(axis, split, gathered, *outs):
    peers, high, lanes = gathered.shape
    row = lax.broadcasted_iota(jnp.int32, (high, lanes), 0)
    before = jnp.where(row >= high // 2, lax.rem(lax.axis_index(axis), peers), 0)
    own, whole = outs[:split], outs[split:]
    counts = [before] + [jnp.where(row >= high // 2, peers, 0)] * bool(whole)
    found = [[] for _ in counts]
    for first in range(0, peers, 8):
        for count, links in zip(counts, found):
            kept = ended = None
            for p in range(first, min(first + 8, peers)):
                t = gathered[p]
                k = jnp.where(p < count, pltpu.roll(t, high // 2, 0), 1.0)
                t = jnp.where(p < count, t, 0.0)
                ended = t if ended is None else ended * k + t
                kept = k if kept is None else kept * k
            links.append((kept, ended))
    for links, out in zip(found, (own, whole)):
        kept, ended = links[0]
        for k, e in links[1:]:
            kept, ended = kept * k, ended * k + e
        for ref, value in zip(out[::-1], (ended, kept)):
            ref[...] = value


def carry_kernel(drop, inner, marks, start, forward, message):
    length, width = drop.shape
    blocks, _, lanes = marks.shape
    groups = width // lanes
    block = length // blocks
    row = lax.broadcasted_iota(jnp.int32, (8, lanes), 0)
    state = start[...]
    ones = jnp.ones((8, lanes), BF16)
    out = jnp.zeros((8, lanes), F32)
    for b in range(blocks):
        rows = pl.ds(b * block, block)
        power = None
        for g in range(groups):
            at = pl.ds(g * lanes, lanes)
            f = inner[rows, at] + state[groups + g : groups + g + 1, :]
            f = f + f * drop[rows, at].astype(F32)
            forward[rows, at] = f
            power = f * f if power is None else power + f * f
        sums = sum(
            lax.dot_general(ones, t, (((1,), (1,)), ((), ())), preferred_element_type=F32)
            for t in pieces(power)
        )
        out = jnp.where(row == b, sums, out)
        state = state * pltpu.roll(marks[b], groups, 0) + marks[b]
    for p in range(message.shape[0]):
        message[p] = out


def norm_kernel(channels, total_length, forward, powers, gain, out, staged, sems):
    length, width = forward.shape
    lanes = powers.shape[-1]
    power = powers[0]
    for p in range(1, powers.shape[0]):
        power = power + powers[p]
    scale = lax.rsqrt(power * (1.0 / (channels * total_length)) + 1e-06) * total_length ** (-0.5)
    scale = scale.T
    copies = []
    for s in range(length // lanes):
        rows = pl.ds(s * lanes, lanes)
        staged[rows, :] = (forward[rows, :] * scale[:, s : s + 1] * gain[...]).astype(BF16)
        copies.append(pltpu.make_async_copy(staged.at[rows], out.at[rows], sems.at[s]))
        copies[-1].start()
    for copy in copies:
        copy.wait()


def per_device(fade_rate, update_in, norm_gain):
    _, length, width = fade_rate.shape
    stretches, parts = lax.axis_size("sp"), lax.axis_size("tp")
    total_length = length * stretches
    rate = LOG2E / total_length
    block, stage = LANES, 512
    half, quarter = stretches // 2, stretches // 4
    blocks = length // block
    limit = pltpu.CompilerParams(vmem_limit_bytes=24 * 1024 * 1024)
    wide = jax.ShapeDtypeStruct((length, width), F32)

    def tiles(count):
        return jax.ShapeDtypeStruct((count, 8, LANES), F32)

    tile = jax.ShapeDtypeStruct((8, LANES), F32)
    drop, inner, marks, summary = pl.pallas_call(
        functools.partial(local_kernel, block, stage, rate),
        out_shape=(jax.ShapeDtypeStruct((length, width), BF16), wide, tiles(blocks), tile),
        in_specs=[HBM, HBM],
        out_specs=(VMEM,) * 4,
        scratch_shapes=[
            pltpu.VMEM((length, width), F32),
            pltpu.VMEM((length, width), BF16),
            pltpu.SemaphoreType.DMA((2, length // stage)),
        ],
        compiler_params=limit,
        name="local",
    )(*(pltpu.with_memory_space_constraint(a[0], pltpu.HBM) for a in (fade_rate, update_in)))
    me = lax.axis_index("sp")

    def within(size, own, whole):
        groups = [list(range(at, at + size)) for at in range(0, stretches, size)]
        prefix = pl.pallas_call(
            functools.partial(prefix_kernel, "sp", own),
            out_shape=(tile,) * (own + whole),
            in_specs=[VMEM],
            out_specs=(VMEM,) * (own + whole),
            compiler_params=limit,
            name="prefix",
        )

        def found(summary, *_):
            copies = jnp.broadcast_to(summary, (size, *summary.shape))
            return prefix(
                lax.all_to_all(copies, "sp", 0, 0, axis_index_groups=groups, tiled=True)
            )

        return found

    def early_half(summary):
        end, first = lax.cond(
            me < quarter, within(quarter, 1, 1), lambda s: (s, s), summary
        )
        start = lax.ppermute(first, "sp", [(i, i + quarter) for i in range(quarter)])
        keep, end, kept, ended = lax.cond(
            me < quarter,
            lambda s, end: (s, end, s, s),
            within(quarter, 2, 2),
            summary,
            end,
        )
        return start * keep + end, start * kept + ended

    def after_first_quarter(summary, state, second):
        start = sum(
            lax.ppermute(second, "sp", pairs)
            for pairs in (
                [(quarter + i, 2 * quarter + i) for i in range(quarter)],
                [(quarter + i, 3 * quarter + (i + quarter // 2) % quarter) for i in range(quarter)],
            )
        )
        keep, end = lax.cond(
            me < half, lambda summary, state: (summary, state), within(half, 2, 0), summary, state
        )
        return start * keep + end

    state, second = lax.cond(me < half, early_half, lambda s: (s, s), summary)
    state = lax.cond(
        me < quarter, lambda _, state, *__: state, after_first_quarter, summary, state, second
    )
    state = pltpu.with_memory_space_constraint(state, pltpu.VMEM)
    forward, power = pl.pallas_call(
        carry_kernel,
        out_shape=(wide, tiles(parts)),
        in_specs=[VMEM] * 4,
        out_specs=(VMEM, VMEM),
        compiler_params=limit,
        name="carry",
    )(drop, inner, marks, state)
    powers = lax.all_to_all(power, "tp", 0, 0, tiled=True)
    out = pl.pallas_call(
        functools.partial(norm_kernel, width * parts, total_length),
        out_shape=jax.ShapeDtypeStruct((length, width), BF16),
        in_specs=[VMEM, VMEM, VMEM],
        out_specs=HBM,
        scratch_shapes=[
            pltpu.VMEM((length, width), BF16),
            pltpu.SemaphoreType.DMA((length // LANES,)),
        ],
        compiler_params=limit,
        name="norm",
    )(forward, powers, norm_gain[None])
    return out[None]


def solution(mesh):
    placed = (P(None, "sp", "tp"), P(None, "sp", "tp"), P("tp"))
    return jax.shard_map(
        per_device, mesh=mesh, in_specs=placed, out_specs=P(None, "sp", "tp"), check_vma=False
    )
```

```python
import functools
import math

import jax
import jax.numpy as jnp
from jax import lax
from jax.experimental import pallas as pl
from jax.experimental.pallas import tpu as pltpu
from jax.sharding import PartitionSpec as P

LANES = 128
F32, BF16 = jnp.float32, jnp.bfloat16
VMEM = pl.BlockSpec(memory_space=pltpu.VMEM)
HBM = pl.BlockSpec(memory_space=pltpu.HBM)
LOG2E = math.log2(math.e)


def pieces(x):
    high = x.astype(BF16)
    return high, (x - high.astype(F32)).astype(BF16)


def as_tile(*rows):
    lines = [r[:, at : at + LANES] for r in rows for at in range(0, r.shape[1], LANES)]
    return jnp.concatenate(lines, axis=0)


def local_kernel(block, stage, rate, fade, update, drop, inner, marks, message, fades, updates, sems):
    length, width = fade.shape
    half = 2 * LANES
    copies = []
    for b in range(length // stage):
        rows = pl.ds(b * stage, stage)
        pair = (
            pltpu.make_async_copy(fade.at[rows], fades.at[rows], sems.at[0, b]),
            pltpu.make_async_copy(update.at[rows], updates.at[rows], sems.at[1, b]),
        )
        for copy in pair:
            copy.start()
        copies.append(pair)
    row = lax.broadcasted_iota(jnp.int32, (block, block), 0)
    column = lax.broadcasted_iota(jnp.int32, (block, block), 1)
    upto = jnp.where(column <= row, 1.0, 0.0).astype(BF16)
    twice = jnp.concatenate([upto, upto], axis=1)

    kept, ended = None, None
    for b in range(length // block):
        rows = pl.ds(b * block, block)
        if b * block % stage == 0:
            for copy in copies[b * block // stage]:
                copy.wait()
        keeps, ends = [], []
        for h in range(width // half):
            at = pl.ds(h * half, half)
            f = fades[rows, at]
            total = jnp.dot(upto, f.astype(BF16), preferred_element_type=F32) * rate
            drop[rows, at] = (jnp.exp2(-total) - 1.0).astype(BF16)
            u = updates[rows, at]
            more = (u.astype(F32) * (jnp.exp2(total) - 1.0)).astype(BF16)
            so_far = jnp.dot(twice, jnp.concatenate([u, more], axis=0), preferred_element_type=F32)
            inner[rows, at] = so_far
            keep = jnp.exp2(jnp.sum(f, axis=0, keepdims=True) * -rate)
            keeps.append(keep)
            ends.append(so_far[block - 1 :, :] * keep)
        keep, end = (jnp.concatenate(r, axis=1) for r in (keeps, ends))
        marks[b] = as_tile(keep, end)
        kept, ended = (keep, end) if kept is None else (kept * keep, ended * keep + end)
    message[...] = as_tile(kept, ended)


def prefix_kernel(axis, split, gathered, *outs):
    peers, high, lanes = gathered.shape
    row = lax.broadcasted_iota(jnp.int32, (high, lanes), 0)
    before = jnp.where(row >= high // 2, lax.rem(lax.axis_index(axis), peers), 0)
    own, whole = outs[:split], outs[split:]
    counts = [before] + [jnp.where(row >= high // 2, peers, 0)] * bool(whole)
    found = [[] for _ in counts]
    for first in range(0, peers, 8):
        for count, links in zip(counts, found):
            kept = ended = None
            for p in range(first, min(first + 8, peers)):
                t = gathered[p]
                k = jnp.where(p < count, pltpu.roll(t, high // 2, 0), 1.0)
                t = jnp.where(p < count, t, 0.0)
                ended = t if ended is None else ended * k + t
                kept = k if kept is None else kept * k
            links.append((kept, ended))
    for links, out in zip(found, (own, whole)):
        kept, ended = links[0]
        for k, e in links[1:]:
            kept, ended = kept * k, ended * k + e
        for ref, value in zip(out[::-1], (ended, kept)):
            ref[...] = value


def carry_kernel(drop, inner, marks, start, forward, message):
    length, width = drop.shape
    blocks, _, lanes = marks.shape
    groups = width // lanes
    block = length // blocks
    row = lax.broadcasted_iota(jnp.int32, (8, lanes), 0)
    state = start[...]
    ones = jnp.ones((8, lanes), BF16)
    out = jnp.zeros((8, lanes), F32)
    for b in range(blocks):
        rows = pl.ds(b * block, block)
        power = None
        for g in range(groups):
            at = pl.ds(g * lanes, lanes)
            f = inner[rows, at] + state[groups + g : groups + g + 1, :]
            f = f + f * drop[rows, at].astype(F32)
            forward[rows, at] = f
            power = f * f if power is None else power + f * f
        sums = sum(
            lax.dot_general(ones, t, (((1,), (1,)), ((), ())), preferred_element_type=F32)
            for t in pieces(power)
        )
        out = jnp.where(row == b, sums, out)
        state = state * pltpu.roll(marks[b], groups, 0) + marks[b]
    for p in range(message.shape[0]):
        message[p] = out


def norm_kernel(channels, total_length, forward, powers, gain, out, staged, sems):
    length, width = forward.shape
    lanes = powers.shape[-1]
    power = powers[0]
    for p in range(1, powers.shape[0]):
        power = power + powers[p]
    scale = lax.rsqrt(power * (1.0 / (channels * total_length)) + 1e-06) * total_length ** (-0.5)
    scale = scale.T
    copies = []
    for s in range(length // lanes):
        rows = pl.ds(s * lanes, lanes)
        staged[rows, :] = (forward[rows, :] * scale[:, s : s + 1] * gain[...]).astype(BF16)
        copies.append(pltpu.make_async_copy(staged.at[rows], out.at[rows], sems.at[s]))
        copies[-1].start()
    for copy in copies:
        copy.wait()


def per_device(fade_rate, update_in, norm_gain):
    _, length, width = fade_rate.shape
    stretches, parts = lax.axis_size("sp"), lax.axis_size("tp")
    total_length = length * stretches
    rate = LOG2E / total_length
    block, stage = LANES, 512
    half, quarter = stretches // 2, stretches // 4
    blocks = length // block
    limit = pltpu.CompilerParams(vmem_limit_bytes=24 * 1024 * 1024)
    wide = jax.ShapeDtypeStruct((length, width), F32)

    def tiles(count):
        return jax.ShapeDtypeStruct((count, 8, LANES), F32)

    tile = jax.ShapeDtypeStruct((8, LANES), F32)
    drop, inner, marks, summary = pl.pallas_call(
        functools.partial(local_kernel, block, stage, rate),
        out_shape=(jax.ShapeDtypeStruct((length, width), BF16), wide, tiles(blocks), tile),
        in_specs=[HBM, HBM],
        out_specs=(VMEM,) * 4,
        scratch_shapes=[
            pltpu.VMEM((length, width), F32),
            pltpu.VMEM((length, width), BF16),
            pltpu.SemaphoreType.DMA((2, length // stage)),
        ],
        compiler_params=limit,
        name="local",
    )(*(pltpu.with_memory_space_constraint(a[0], pltpu.HBM) for a in (fade_rate, update_in)))
    me = lax.axis_index("sp")

    def within(size, own, whole):
        groups = [list(range(at, at + size)) for at in range(0, stretches, size)]
        prefix = pl.pallas_call(
            functools.partial(prefix_kernel, "sp", own),
            out_shape=(tile,) * (own + whole),
            in_specs=[VMEM],
            out_specs=(VMEM,) * (own + whole),
            compiler_params=limit,
            name="prefix",
        )

        def found(summary, *_):
            copies = jnp.broadcast_to(summary, (size, *summary.shape))
            return prefix(
                lax.all_to_all(copies, "sp", 0, 0, axis_index_groups=groups, tiled=True)
            )

        return found

    def early_half(summary):
        end, first = lax.cond(
            me < quarter, within(quarter, 1, 1), lambda s: (s, s), summary
        )
        start = lax.ppermute(first, "sp", [(i, quarter + (i + quarter // 2) % quarter) for i in range(quarter)])
        keep, end, kept, ended = lax.cond(
            me < quarter,
            lambda s, end: (s, end, s, s),
            within(quarter, 2, 2),
            summary,
            end,
        )
        return start * keep + end, start * kept + ended

    def after_first_quarter(summary, state, second):
        start = sum(
            lax.ppermute(second, "sp", pairs)
            for pairs in (
                [(quarter + i, 2 * quarter + i) for i in range(quarter)],
                [(quarter + i, 3 * quarter + (i + quarter // 2) % quarter) for i in range(quarter)],
            )
        )
        keep, end = lax.cond(
            me < half, lambda summary, state: (summary, state), within(half, 2, 0), summary, state
        )
        return start * keep + end

    state, second = lax.cond(me < half, early_half, lambda s: (s, s), summary)
    state = lax.cond(
        me < quarter, lambda _, state, *__: state, after_first_quarter, summary, state, second
    )
    state = pltpu.with_memory_space_constraint(state, pltpu.VMEM)
    forward, power = pl.pallas_call(
        carry_kernel,
        out_shape=(wide, tiles(parts)),
        in_specs=[VMEM] * 4,
        out_specs=(VMEM, VMEM),
        compiler_params=limit,
        name="carry",
    )(drop, inner, marks, state)
    powers = lax.all_to_all(power, "tp", 0, 0, tiled=True)
    out = pl.pallas_call(
        functools.partial(norm_kernel, width * parts, total_length),
        out_shape=jax.ShapeDtypeStruct((length, width), BF16),
        in_specs=[VMEM, VMEM, VMEM],
        out_specs=HBM,
        scratch_shapes=[
            pltpu.VMEM((length, width), BF16),
            pltpu.SemaphoreType.DMA((length // LANES,)),
        ],
        compiler_params=limit,
        name="norm",
    )(forward, powers, norm_gain[None])
    return out[None]


def solution(mesh):
    placed = (P(None, "sp", "tp"), P(None, "sp", "tp"), P("tp"))
    return jax.shard_map(
        per_device, mesh=mesh, in_specs=placed, out_specs=P(None, "sp", "tp"), check_vma=False
    )
```

```python
import functools
import math

import jax
import jax.numpy as jnp
from jax import lax
from jax.experimental import pallas as pl
from jax.experimental.pallas import tpu as pltpu
from jax.sharding import PartitionSpec as P

LANES = 128
F32, BF16 = jnp.float32, jnp.bfloat16
VMEM = pl.BlockSpec(memory_space=pltpu.VMEM)
HBM = pl.BlockSpec(memory_space=pltpu.HBM)
LOG2E = math.log2(math.e)


def pieces(x):
    high = x.astype(BF16)
    return high, (x - high.astype(F32)).astype(BF16)


def as_tile(*rows):
    lines = [r[:, at : at + LANES] for r in rows for at in range(0, r.shape[1], LANES)]
    return jnp.concatenate(lines, axis=0)


def local_kernel(block, stages, rate, fade, update, drop, inner, marks, message, fades, updates, sems):
    length, width = fade.shape
    half = 2 * LANES
    copies = []
    for b, (at, to) in enumerate(zip(stages, (*stages[1:], length))):
        rows = pl.ds(at, to - at)
        pair = (
            pltpu.make_async_copy(fade.at[rows], fades.at[rows], sems.at[0, b]),
            pltpu.make_async_copy(update.at[rows], updates.at[rows], sems.at[1, b]),
        )
        for copy in pair:
            copy.start()
        copies.append(pair)
    row = lax.broadcasted_iota(jnp.int32, (block, block), 0)
    column = lax.broadcasted_iota(jnp.int32, (block, block), 1)
    upto = jnp.where(column <= row, 1.0, 0.0).astype(BF16)
    twice = jnp.concatenate([upto, upto], axis=1)

    kept, ended = None, None
    for b in range(length // block):
        rows = pl.ds(b * block, block)
        if b * block in stages:
            for copy in copies[stages.index(b * block)]:
                copy.wait()
        keeps, ends = [], []
        for h in range(width // half):
            at = pl.ds(h * half, half)
            f = fades[rows, at]
            total = jnp.dot(upto, f.astype(BF16), preferred_element_type=F32) * rate
            drop[rows, at] = (jnp.exp2(-total) - 1.0).astype(BF16)
            u = updates[rows, at]
            more = (u.astype(F32) * (jnp.exp2(total) - 1.0)).astype(BF16)
            so_far = jnp.dot(twice, jnp.concatenate([u, more], axis=0), preferred_element_type=F32)
            inner[rows, at] = so_far
            keep = jnp.exp2(jnp.sum(f, axis=0, keepdims=True) * -rate)
            keeps.append(keep)
            ends.append(so_far[block - 1 :, :] * keep)
        keep, end = (jnp.concatenate(r, axis=1) for r in (keeps, ends))
        marks[b] = as_tile(keep, end)
        kept, ended = (keep, end) if kept is None else (kept * keep, ended * keep + end)
    message[...] = as_tile(kept, ended)


def prefix_kernel(axis, split, gathered, *outs):
    peers, high, lanes = gathered.shape
    row = lax.broadcasted_iota(jnp.int32, (high, lanes), 0)
    before = jnp.where(row >= high // 2, lax.rem(lax.axis_index(axis), peers), 0)
    own, whole = outs[:split], outs[split:]
    counts = [before] + [jnp.where(row >= high // 2, peers, 0)] * bool(whole)
    found = [[] for _ in counts]
    for first in range(0, peers, 8):
        for count, links in zip(counts, found):
            kept = ended = None
            for p in range(first, min(first + 8, peers)):
                t = gathered[p]
                k = jnp.where(p < count, pltpu.roll(t, high // 2, 0), 1.0)
                t = jnp.where(p < count, t, 0.0)
                ended = t if ended is None else ended * k + t
                kept = k if kept is None else kept * k
            links.append((kept, ended))
    for links, out in zip(found, (own, whole)):
        kept, ended = links[0]
        for k, e in links[1:]:
            kept, ended = kept * k, ended * k + e
        for ref, value in zip(out[::-1], (ended, kept)):
            ref[...] = value


def carry_kernel(drop, inner, marks, start, forward, message):
    length, width = drop.shape
    blocks, _, lanes = marks.shape
    groups = width // lanes
    block = length // blocks
    row = lax.broadcasted_iota(jnp.int32, (8, lanes), 0)
    state = start[...]
    ones = jnp.ones((8, lanes), BF16)
    out = jnp.zeros((8, lanes), F32)
    for b in range(blocks):
        rows = pl.ds(b * block, block)
        power = None
        for g in range(groups):
            at = pl.ds(g * lanes, lanes)
            f = inner[rows, at] + state[groups + g : groups + g + 1, :]
            f = f + f * drop[rows, at].astype(F32)
            forward[rows, at] = f
            power = f * f if power is None else power + f * f
        sums = sum(
            lax.dot_general(ones, t, (((1,), (1,)), ((), ())), preferred_element_type=F32)
            for t in pieces(power)
        )
        out = jnp.where(row == b, sums, out)
        state = state * pltpu.roll(marks[b], groups, 0) + marks[b]
    for p in range(message.shape[0]):
        message[p] = out


def norm_kernel(channels, total_length, forward, powers, gain, out, staged, sems):
    length, width = forward.shape
    lanes = powers.shape[-1]
    power = powers[0]
    for p in range(1, powers.shape[0]):
        power = power + powers[p]
    scale = lax.rsqrt(power * (1.0 / (channels * total_length)) + 1e-06) * total_length ** (-0.5)
    scale = scale.T
    copies = []
    for s in range(length // lanes):
        rows = pl.ds(s * lanes, lanes)
        staged[rows, :] = (forward[rows, :] * scale[:, s : s + 1] * gain[...]).astype(BF16)
        copies.append(pltpu.make_async_copy(staged.at[rows], out.at[rows], sems.at[s]))
        copies[-1].start()
    for copy in copies:
        copy.wait()


def per_device(fade_rate, update_in, norm_gain):
    _, length, width = fade_rate.shape
    stretches, parts = lax.axis_size("sp"), lax.axis_size("tp")
    total_length = length * stretches
    rate = LOG2E / total_length
    block, stages = LANES, (0, 384)
    half, quarter = stretches // 2, stretches // 4
    blocks = length // block
    limit = pltpu.CompilerParams(vmem_limit_bytes=24 * 1024 * 1024)
    wide = jax.ShapeDtypeStruct((length, width), F32)

    def tiles(count):
        return jax.ShapeDtypeStruct((count, 8, LANES), F32)

    tile = jax.ShapeDtypeStruct((8, LANES), F32)
    drop, inner, marks, summary = pl.pallas_call(
        functools.partial(local_kernel, block, stages, rate),
        out_shape=(jax.ShapeDtypeStruct((length, width), BF16), wide, tiles(blocks), tile),
        in_specs=[HBM, HBM],
        out_specs=(VMEM,) * 4,
        scratch_shapes=[
            pltpu.VMEM((length, width), F32),
            pltpu.VMEM((length, width), BF16),
            pltpu.SemaphoreType.DMA((2, len(stages))),
        ],
        compiler_params=limit,
        name="local",
    )(*(pltpu.with_memory_space_constraint(a[0], pltpu.HBM) for a in (fade_rate, update_in)))
    me = lax.axis_index("sp")

    def within(size, own, whole):
        groups = [list(range(at, at + size)) for at in range(0, stretches, size)]
        prefix = pl.pallas_call(
            functools.partial(prefix_kernel, "sp", own),
            out_shape=(tile,) * (own + whole),
            in_specs=[VMEM],
            out_specs=(VMEM,) * (own + whole),
            compiler_params=limit,
            name="prefix",
        )

        def found(summary, *_):
            copies = jnp.broadcast_to(summary, (size, *summary.shape))
            return prefix(
                lax.all_to_all(copies, "sp", 0, 0, axis_index_groups=groups, tiled=True)
            )

        return found

    def early_half(summary):
        end, first = lax.cond(
            me < quarter, within(quarter, 1, 1), lambda s: (s, s), summary
        )
        start = lax.ppermute(first, "sp", [(i, quarter + (i + quarter // 2) % quarter) for i in range(quarter)])
        keep, end, kept, ended = lax.cond(
            me < quarter,
            lambda s, end: (s, end, s, s),
            within(quarter, 2, 2),
            summary,
            end,
        )
        return start * keep + end, start * kept + ended

    def after_first_quarter(summary, state, second):
        start = sum(
            lax.ppermute(second, "sp", pairs)
            for pairs in (
                [(quarter + i, 2 * quarter + (i + quarter // 2) % quarter) for i in range(quarter)],
                [(quarter + i, 3 * quarter + (i + quarter // 2) % quarter) for i in range(quarter)],
            )
        )
        keep, end = lax.cond(
            me < half, lambda summary, state: (summary, state), within(half, 2, 0), summary, state
        )
        return start * keep + end

    state, second = lax.cond(me < half, early_half, lambda s: (s, s), summary)
    state = lax.cond(
        me < quarter, lambda _, state, *__: state, after_first_quarter, summary, state, second
    )
    state = pltpu.with_memory_space_constraint(state, pltpu.VMEM)
    forward, power = pl.pallas_call(
        carry_kernel,
        out_shape=(wide, tiles(parts)),
        in_specs=[VMEM] * 4,
        out_specs=(VMEM, VMEM),
        compiler_params=limit,
        name="carry",
    )(drop, inner, marks, state)
    powers = lax.all_to_all(power, "tp", 0, 0, tiled=True)
    out = pl.pallas_call(
        functools.partial(norm_kernel, width * parts, total_length),
        out_shape=jax.ShapeDtypeStruct((length, width), BF16),
        in_specs=[VMEM, VMEM, VMEM],
        out_specs=HBM,
        scratch_shapes=[
            pltpu.VMEM((length, width), BF16),
            pltpu.SemaphoreType.DMA((length // LANES,)),
        ],
        compiler_params=limit,
        name="norm",
    )(forward, powers, norm_gain[None])
    return out[None]


def solution(mesh):
    placed = (P(None, "sp", "tp"), P(None, "sp", "tp"), P("tp"))
    return jax.shard_map(
        per_device, mesh=mesh, in_specs=placed, out_specs=P(None, "sp", "tp"), check_vma=False
    )
```

```python
import functools
import math

import jax
import jax.numpy as jnp
from jax import lax
from jax.experimental import pallas as pl
from jax.experimental.pallas import tpu as pltpu
from jax.sharding import PartitionSpec as P

LANES = 128
F32, BF16 = jnp.float32, jnp.bfloat16
VMEM = pl.BlockSpec(memory_space=pltpu.VMEM)
HBM = pl.BlockSpec(memory_space=pltpu.HBM)
LOG2E = math.log2(math.e)


def pieces(x):
    high = x.astype(BF16)
    return high, (x - high.astype(F32)).astype(BF16)


def as_tile(*rows):
    lines = [r[:, at : at + LANES] for r in rows for at in range(0, r.shape[1], LANES)]
    return jnp.concatenate(lines, axis=0)


def local_kernel(block, stages, rate, fade, update, drop, inner, marks, message, fades, updates, sems):
    length, width = fade.shape
    half = 2 * LANES
    copies = []
    for b, (at, to) in enumerate(zip(stages, (*stages[1:], length))):
        rows = pl.ds(at, to - at)
        pair = (
            pltpu.make_async_copy(fade.at[rows], fades.at[rows], sems.at[0, b]),
            pltpu.make_async_copy(update.at[rows], updates.at[rows], sems.at[1, b]),
        )
        for copy in pair:
            copy.start()
        copies.append(pair)
    row = lax.broadcasted_iota(jnp.int32, (block, block), 0)
    column = lax.broadcasted_iota(jnp.int32, (block, block), 1)
    upto = jnp.where(column <= row, 1.0, 0.0).astype(BF16)
    twice = jnp.concatenate([upto, upto], axis=1)

    kept, ended = None, None
    for b in range(length // block):
        rows = pl.ds(b * block, block)
        if b * block in stages:
            for copy in copies[stages.index(b * block)]:
                copy.wait()
        keeps, ends = [], []
        for h in range(width // half):
            at = pl.ds(h * half, half)
            f = fades[rows, at]
            total = jnp.dot(upto, f.astype(BF16), preferred_element_type=F32) * rate
            drop[rows, at] = (jnp.exp2(-total) - 1.0).astype(BF16)
            u = updates[rows, at]
            more = (u.astype(F32) * (jnp.exp2(total) - 1.0)).astype(BF16)
            so_far = jnp.dot(twice, jnp.concatenate([u, more], axis=0), preferred_element_type=F32)
            inner[rows, at] = so_far
            keep = jnp.exp2(jnp.sum(f, axis=0, keepdims=True) * -rate)
            keeps.append(keep)
            ends.append(so_far[block - 1 :, :] * keep)
        keep, end = (jnp.concatenate(r, axis=1) for r in (keeps, ends))
        marks[b] = as_tile(keep, end)
        kept, ended = (keep, end) if kept is None else (kept * keep, ended * keep + end)
    message[...] = as_tile(kept, ended)


def prefix_kernel(axis, split, gathered, *outs):
    peers, high, lanes = gathered.shape
    row = lax.broadcasted_iota(jnp.int32, (high, lanes), 0)
    before = jnp.where(row >= high // 2, lax.rem(lax.axis_index(axis), peers), 0)
    own, whole = outs[:split], outs[split:]
    counts = [before] + [jnp.where(row >= high // 2, peers, 0)] * bool(whole)
    found = [[] for _ in counts]
    for first in range(0, peers, 8):
        for count, links in zip(counts, found):
            kept = ended = None
            for p in range(first, min(first + 8, peers)):
                t = gathered[p]
                k = jnp.where(p < count, pltpu.roll(t, high // 2, 0), 1.0)
                t = jnp.where(p < count, t, 0.0)
                ended = t if ended is None else ended * k + t
                kept = k if kept is None else kept * k
            links.append((kept, ended))
    for links, out in zip(found, (own, whole)):
        kept, ended = links[0]
        for k, e in links[1:]:
            kept, ended = kept * k, ended * k + e
        for ref, value in zip(out[::-1], (ended, kept)):
            ref[...] = value


def carry_kernel(drop, inner, marks, start, forward, message):
    length, width = drop.shape
    blocks, _, lanes = marks.shape
    groups = width // lanes
    block = length // blocks
    row = lax.broadcasted_iota(jnp.int32, (8, lanes), 0)
    state = start[...]
    ones = jnp.ones((8, lanes), BF16)
    out = jnp.zeros((8, lanes), F32)
    for b in range(blocks):
        rows = pl.ds(b * block, block)
        power = None
        for g in range(groups):
            at = pl.ds(g * lanes, lanes)
            f = inner[rows, at] + state[groups + g : groups + g + 1, :]
            f = f + f * drop[rows, at].astype(F32)
            forward[rows, at] = f
            power = f * f if power is None else power + f * f
        sums = sum(
            lax.dot_general(ones, t, (((1,), (1,)), ((), ())), preferred_element_type=F32)
            for t in pieces(power)
        )
        out = jnp.where(row == b, sums, out)
        state = state * pltpu.roll(marks[b], groups, 0) + marks[b]
    for p in range(message.shape[0]):
        message[p] = out


def norm_kernel(channels, total_length, forward, powers, gain, out, staged, sems):
    length, width = forward.shape
    lanes = powers.shape[-1]
    power = powers[0]
    for p in range(1, powers.shape[0]):
        power = power + powers[p]
    scale = lax.rsqrt(power * (1.0 / (channels * total_length)) + 1e-06) * total_length ** (-0.5)
    scale = scale.T
    copies = []
    for s in range(length // lanes):
        rows = pl.ds(s * lanes, lanes)
        staged[rows, :] = (forward[rows, :] * scale[:, s : s + 1] * gain[...]).astype(BF16)
        if s % 2:
            pair = pl.ds((s - 1) * lanes, 2 * lanes)
            copies.append(pltpu.make_async_copy(staged.at[pair], out.at[pair], sems.at[s // 2]))
            copies[-1].start()
    for copy in copies:
        copy.wait()


def per_device(fade_rate, update_in, norm_gain):
    _, length, width = fade_rate.shape
    stretches, parts = lax.axis_size("sp"), lax.axis_size("tp")
    total_length = length * stretches
    rate = LOG2E / total_length
    block, stages = LANES, (0, 384)
    half, quarter = stretches // 2, stretches // 4
    blocks = length // block
    limit = pltpu.CompilerParams(vmem_limit_bytes=24 * 1024 * 1024)
    wide = jax.ShapeDtypeStruct((length, width), F32)

    def tiles(count):
        return jax.ShapeDtypeStruct((count, 8, LANES), F32)

    tile = jax.ShapeDtypeStruct((8, LANES), F32)
    drop, inner, marks, summary = pl.pallas_call(
        functools.partial(local_kernel, block, stages, rate),
        out_shape=(jax.ShapeDtypeStruct((length, width), BF16), wide, tiles(blocks), tile),
        in_specs=[HBM, HBM],
        out_specs=(VMEM,) * 4,
        scratch_shapes=[
            pltpu.VMEM((length, width), F32),
            pltpu.VMEM((length, width), BF16),
            pltpu.SemaphoreType.DMA((2, len(stages))),
        ],
        compiler_params=limit,
        name="local",
    )(*(pltpu.with_memory_space_constraint(a[0], pltpu.HBM) for a in (fade_rate, update_in)))
    me = lax.axis_index("sp")

    def within(size, own, whole):
        groups = [list(range(at, at + size)) for at in range(0, stretches, size)]
        prefix = pl.pallas_call(
            functools.partial(prefix_kernel, "sp", own),
            out_shape=(tile,) * (own + whole),
            in_specs=[VMEM],
            out_specs=(VMEM,) * (own + whole),
            compiler_params=limit,
            name="prefix",
        )

        def found(summary, *_):
            copies = jnp.broadcast_to(summary, (size, *summary.shape))
            return prefix(
                lax.all_to_all(copies, "sp", 0, 0, axis_index_groups=groups, tiled=True)
            )

        return found

    def early_half(summary):
        end, first = lax.cond(
            me < quarter, within(quarter, 1, 1), lambda s: (s, s), summary
        )
        start = lax.ppermute(first, "sp", [(i, quarter + (i + quarter // 2) % quarter) for i in range(quarter)])
        keep, end, kept, ended = lax.cond(
            me < quarter,
            lambda s, end: (s, end, s, s),
            within(quarter, 2, 2),
            summary,
            end,
        )
        return start * keep + end, start * kept + ended

    def after_first_quarter(summary, state, second):
        start = sum(
            lax.ppermute(second, "sp", pairs)
            for pairs in (
                [(quarter + i, 2 * quarter + (i + quarter // 2) % quarter) for i in range(quarter)],
                [(quarter + i, 3 * quarter + (i + quarter // 2) % quarter) for i in range(quarter)],
            )
        )
        keep, end = lax.cond(
            me < half, lambda summary, state: (summary, state), within(half, 2, 0), summary, state
        )
        return start * keep + end

    state, second = lax.cond(me < half, early_half, lambda s: (s, s), summary)
    state = lax.cond(
        me < quarter, lambda _, state, *__: state, after_first_quarter, summary, state, second
    )
    state = pltpu.with_memory_space_constraint(state, pltpu.VMEM)
    forward, power = pl.pallas_call(
        carry_kernel,
        out_shape=(wide, tiles(parts)),
        in_specs=[VMEM] * 4,
        out_specs=(VMEM, VMEM),
        compiler_params=limit,
        name="carry",
    )(drop, inner, marks, state)
    powers = lax.all_to_all(power, "tp", 0, 0, tiled=True)
    out = pl.pallas_call(
        functools.partial(norm_kernel, width * parts, total_length),
        out_shape=jax.ShapeDtypeStruct((length, width), BF16),
        in_specs=[VMEM, VMEM, VMEM],
        out_specs=HBM,
        scratch_shapes=[
            pltpu.VMEM((length, width), BF16),
            pltpu.SemaphoreType.DMA((length // LANES // 2,)),
        ],
        compiler_params=limit,
        name="norm",
    )(forward, powers, norm_gain[None])
    return out[None]


def solution(mesh):
    placed = (P(None, "sp", "tp"), P(None, "sp", "tp"), P("tp"))
    return jax.shard_map(
        per_device, mesh=mesh, in_specs=placed, out_specs=P(None, "sp", "tp"), check_vma=False
    )
```
